32 devices in a mesh: grp: 8 (over y, x, core), sp: 4 (over z).
Axes of the slice: x: 2, y: 2, z: 4, core: 2. Of those that a mesh axis runs over, the one named last changes fastest.
Arguments:
- latents: bfloat16 [8, 512, 3072], P('grp', 'sp'), may hold values from -6 to 6
- timestep: int32 [8], P('grp'), may hold values from 0 to 999
- w_mod: bfloat16 [256, 9216], replicated, may hold values from -0.375 to 0.375
- w_qkv: bfloat16 [4, 3072, 384], P('sp', 'grp'), may hold values from -2 to 2
- w_out: bfloat16 [4, 128, 3072], P('sp', 'grp'), may hold values from -0.5 to 0.5
Outputs:
- update: bfloat16 [8, 512, 3072], P('grp', 'sp')
The draws below stay inside these ranges and needn't reach their ends.
All inputs are finite; a program needn't handle non-finite values.
Results may differ from the reference program's by a relative error of at most 0.012.
Values may be sent and summed in bfloat16 or wider, within the bound.
A program may use at most 128 MiB of HBM per device.

```python
import math
import jax
import jax.numpy as jnp
from jax import lax

D = 3072
HS = 128
FREQ = 256
H = 4
LEN = 512
IMAGES = 8


def draw_w_qkv(key, part):
    first, second, third = jax.random.split(jax.random.fold_in(key, 17), 3)
    base = 1.0 / math.sqrt(D)
    query_part = jax.random.normal(first, (H, D, HS), jnp.float32) * (1.5 * base)
    value_part = jax.random.normal(third, (H, D, HS), jnp.float32) * base
    key_part = jax.random.normal(second, (H, D, HS), jnp.float32) * base
    whole = jnp.concatenate([query_part, key_part, value_part], axis=2)
    return jnp.clip(whole, -2.0, 2.0).astype(jnp.bfloat16)


def plant(array, stream_key, smallest, top_value):
    spot = [jax.random.randint(jax.random.fold_in(stream_key, axis), (), 0, length) for axis, length in enumerate(array.shape)]
    main_axis = array.shape.index(max(array.shape))
    next_to = spot[:main_axis] + [(spot[main_axis] + 1) % array.shape[main_axis]] + spot[main_axis + 1:]
    return array.at[tuple(spot)].set(smallest).at[tuple(next_to)].set(top_value)


def shard_levels(rng, shape, cuts, low, high):
    level, own = 1.0, jax.random.fold_in(rng, 6)
    for dim, shards_of in cuts:
        steps = jnp.exp(jax.random.uniform(jax.random.fold_in(own, dim), (shards_of,), jnp.float32, low / len(cuts), high / len(cuts)))
        level = level * jnp.repeat(steps, shape[dim] // shards_of).reshape([-1 if axis == dim else 1 for axis in range(len(shape))])
    return level


def centred(stream_key, shape, scale, limit, cuts=(), held_as=jnp.bfloat16):
    array = jax.random.normal(stream_key, shape, jnp.float32) * scale
    if len(cuts) > 0:
        array = shard_levels(stream_key, shape, cuts, -0.22, 0.18) * array
    return jnp.clip(array, min=-limit, max=limit).astype(held_as)


def setup_inputs(seed: int = 0) -> dict:
    arg_keys = jax.random.split(jax.random.key(seed), 6)
    latents = centred(arg_keys[0], (IMAGES, LEN, D), 1.0, 6.0, ((0, 8), (1, 4)))
    timestep = plant(jax.random.randint(arg_keys[1], (IMAGES,), 0, 1000), jax.random.fold_in(arg_keys[1], 1), 0, 999).astype(jnp.int32)
    w_mod = centred(arg_keys[2], (FREQ, 3 * D), FREQ ** -0.5, 0.375)
    w_qkv = draw_w_qkv(jax.random.fold_in(arg_keys[5], 71), 0)
    w_out = centred(arg_keys[4], (H, HS, D), HS ** -0.5, 0.5, ((0, 4), (1, 8)))
    return {"latents": latents, "timestep": timestep, "w_mod": w_mod, "w_qkv": w_qkv, "w_out": w_out}


def modulation(timestep, w_mod):
    half_freq = w_mod.shape[0] // 2
    freqs = jnp.exp(-math.log(10000.0) * jnp.arange(half_freq, dtype=jnp.float32) / half_freq)
    angles = timestep.astype(jnp.float32)[:, None] * freqs[None, :]
    embed = jnp.concatenate([jnp.cos(angles), jnp.sin(angles)], axis=1).astype(jnp.bfloat16)
    return jnp.dot(embed, w_mod, preferred_element_type=jnp.float32)

def normalize(latents, shift, scale):
    values = latents.astype(jnp.float32)
    center = lax.optimization_barrier(jnp.mean(values, axis=-1, keepdims=True))
    spread = lax.optimization_barrier(jnp.mean((values - center) ** 2, axis=-1, keepdims=True))
    normed = (values - center) * lax.rsqrt(spread + 1e-06)
    return (normed * (1.0 + scale[:, None, :]) + shift[:, None, :]).astype(jnp.bfloat16)

def attend(query, keys, values):
    length, head_size = query.shape
    block = min(512, length)
    blocks = query.reshape(length // block, block, head_size)

    def one_block(query_rows):
        scores = lax.dot_general(query_rows, keys, (((1,), (1,)), ((), ())), preferred_element_type=jnp.float32)
        scores = scores / math.sqrt(head_size)
        largest = lax.optimization_barrier(jnp.max(scores, axis=1, keepdims=True))
        weights = jnp.exp(scores - largest)
        probs = (weights / lax.optimization_barrier(jnp.sum(weights, axis=1, keepdims=True))).astype(jnp.bfloat16)
        return jnp.dot(probs, values, preferred_element_type=jnp.float32).astype(jnp.bfloat16)
    return lax.map(one_block, blocks).reshape(length, head_size)

def reference(latents, timestep, w_mod, w_qkv, w_out):
    width = latents.shape[2]
    head_size = w_out.shape[1]
    mod = modulation(timestep, w_mod)
    shift = mod[:, :width]
    scale = mod[:, width:2 * width]
    gate = mod[:, 2 * width:]
    normed = normalize(latents, shift, scale)

    def one_image(inputs):
        normed_one, gate_one = inputs

        def one_head(total, weights):
            weight_in, weight_out = weights
            qkv = jnp.dot(normed_one, weight_in, preferred_element_type=jnp.float32).astype(jnp.bfloat16)
            attended = attend(qkv[:, :head_size], qkv[:, head_size:2 * head_size], qkv[:, 2 * head_size:])
            contrib = jnp.dot(attended, weight_out, preferred_element_type=jnp.float32).astype(jnp.bfloat16)
            contrib = lax.optimization_barrier(contrib)
            return (total + contrib.astype(jnp.float32), None)
        start_total = jnp.zeros((normed_one.shape[0], width), jnp.float32)
        total, unused = lax.scan(one_head, start_total, (w_qkv, w_out))
        return (gate_one[None, :] * total).astype(jnp.bfloat16)
    return lax.map(one_image, (normed, gate))
```

```python
import functools
import math

import jax
import jax.numpy as jnp
from jax import lax
from jax.experimental import pallas as pl
from jax.experimental.pallas import tpu as pltpu
from jax.sharding import PartitionSpec as P

MESH = pl.DeviceIdType.MESH


def embedding(timestep, freq):
    half_freq = freq // 2
    freqs = jnp.exp(-math.log(10000.0) * jnp.arange(half_freq, dtype=jnp.float32) / half_freq)
    angles = timestep.astype(jnp.float32)[:, None] * freqs[None, :]
    return jnp.concatenate([jnp.cos(angles), jnp.sin(angles)], axis=1).astype(jnp.bfloat16)


def kernel(
    n_grp,
    n_sp,
    lat_hbm,
    embed_ref,
    wmod_hbm,
    wqkv_hbm,
    wout_hbm,
    out_ref,
    lat,
    wmod,
    mod,
    normed,
    wq,
    wo,
    q_buf,
    kv,
    att_mine,
    att_send,
    loc_sem,
    wz_s,
    wz_r,
    wx_s,
    wx_r,
    wd_s,
    wd_r,
    oz_s,
    oz_r,
    ox_s,
    ox_r,
    od_s,
    od_r,
    lat_s,
    lat_r,
    kv_s,
    kv_r,
    at_s,
    at_r,
):
    g = lax.axis_index("grp")
    s = lax.axis_index("sp")
    core, chip = g % 2, g // 2
    chips = n_grp // 2
    pairs = n_sp // 2
    parity, pair = s % 2, s // 2
    tok, width = lat_hbm.shape[1], lat_hbm.shape[2]
    rows_q = wqkv_hbm.shape[1]
    rows_o = wout_hbm.shape[1]
    head = wqkv_hbm.shape[2] // 3
    sib = (chip * 2 + 1 - core, s)
    mate = (g, pair * 2 + 1 - parity)

    def at_chip(c):
        return ((chip + c) % chips * 2 + core, s)

    def at_pair(k, flip):
        return (g, (pair + k) % pairs * 2 + (parity + flip) % 2)

    def remote(src, dst, ssem, rsem, device):
        return pltpu.make_async_remote_copy(
            src_ref=src, dst_ref=dst, send_sem=ssem, recv_sem=rsem, device_id=device, device_id_type=MESH
        )

    def wq_rows(k, owner):
        return wq.at[k, pl.ds(pl.multiple_of(owner * rows_q, rows_q), rows_q), :]

    def wo_rows(par, k, owner):
        first = (par * pairs + k) * head + owner * rows_o
        return wo.at[pl.ds(pl.multiple_of(first, rows_o), rows_o), :]

    barrier = pltpu.get_barrier_semaphore()
    peers = [sib] + [at_chip(c) for c in range(1, chips)]
    peers += [at_pair(k, f) for k in range(pairs) for f in range(2) if (k, f) != (0, 0)]
    for peer in peers:
        pl.semaphore_signal(barrier, inc=1, device_id=peer, device_id_type=MESH)
    local = [
        pltpu.make_async_copy(wqkv_hbm.at[0], wq_rows(0, g), loc_sem.at[0]),
        pltpu.make_async_copy(wout_hbm.at[0], wo_rows(parity, 0, g), loc_sem.at[1]),
        pltpu.make_async_copy(lat_hbm.at[0], lat.at[0], loc_sem.at[2]),
        pltpu.make_async_copy(wmod_hbm, wmod, loc_sem.at[3]),
    ]
    for copy in local:
        copy.start()
    local[0].wait()
    local[1].wait()
    local[2].wait()
    pl.semaphore_wait(barrier, len(peers))

    sends = []

    def start(*args):
        copy = remote(*args)
        copy.start()
        sends.append(copy)

    def arrive(region, ssem, rsem):
        remote(region, region, ssem, rsem, sib).wait_recv()

    for k in range(1, pairs):
        start(wq_rows(0, g), wq_rows(k, g), wz_s.at[k], wz_r.at[k], at_pair(k, 0))

    def spread_q(k):
        for c in range(1, chips):
            start(wq_rows(k, g), wq_rows(k, g), wx_s.at[k, c], wx_r.at[k, c], at_chip(c))
        start(wq_rows(k, g), wq_rows(k, g), wd_s.at[k, 0], wd_r.at[k, 0], sib)

    def pass_q(k):
        for c in range(1, chips):
            region = wq_rows(k, (chip + chips - c) % chips * 2 + core)
            arrive(region, wx_s.at[k, c], wx_r.at[k, c])
            start(region, region, wd_s.at[k, c], wd_r.at[k, c], sib)

    def finish_q(k):
        for c in range(chips):
            region = wq_rows(k, (chip + chips - c) % chips * 2 + 1 - core)
            arrive(region, wd_s.at[k, c], wd_r.at[k, c])

    def spread_o(k, flip):
        region = wo_rows((parity + flip) % 2, k, g)
        i = k * 2 + flip
        for c in range(1, chips):
            start(region, region, ox_s.at[i, c], ox_r.at[i, c], at_chip(c))
        start(region, region, od_s.at[i, 0], od_r.at[i, 0], sib)

    def pass_o(k, flip):
        i = k * 2 + flip
        for c in range(1, chips):
            region = wo_rows((parity + flip) % 2, k, (chip + chips - c) % chips * 2 + core)
            arrive(region, ox_s.at[i, c], ox_r.at[i, c])
            start(region, region, od_s.at[i, c], od_r.at[i, c], sib)

    def finish_o(k, flip):
        i = k * 2 + flip
        for c in range(chips):
            region = wo_rows((parity + flip) % 2, k, (chip + chips - c) % chips * 2 + 1 - core)
            arrive(region, od_s.at[i, c], od_r.at[i, c])

    far = [(k, f) for k in range(pairs) for f in range(2) if (k, f) != (0, 0)]

    spread_q(0)
    start(lat.at[0], lat.at[1], lat_s.at[0], lat_r.at[0], mate)
    for k, f in far:
        i = k * 2 + f
        start(wo_rows(parity, 0, g), wo_rows(parity, k, g), oz_s.at[i], oz_r.at[i], at_pair(k, f))
    spread_o(0, 0)

    local[3].wait()
    step = min(512, width)

    @pl.loop(0, 3 * width // step)
    def _(i):
        cols = pl.ds(pl.multiple_of(i * step, step), step)
        part = jnp.dot(embed_ref[...], wmod[:, cols], preferred_element_type=jnp.float32)
        mod[:, cols] = part[:8]

    def normalize(which):
        block = 16

        @pl.loop(0, tok // block)
        def _(i):
            rows = pl.ds(pl.multiple_of(i * block, block), block)
            values = lat[which, rows, :].astype(jnp.float32)
            center = jnp.mean(values, axis=-1, keepdims=True)
            values = values - center
            spread = jnp.mean(values * values, axis=-1, keepdims=True)
            scaled = values * lax.rsqrt(spread + 1e-06)
            shift = mod[0:1, 0:width]
            scale = mod[0:1, width : 2 * width]
            target = pl.ds(pl.multiple_of(which * tok + i * block, block), block)
            normed[target, :] = (scaled * (1.0 + scale) + shift).astype(jnp.bfloat16)

    def project(k, first, count):
        rows = pl.ds(first, count)
        result = jnp.dot(normed[rows, :], wq[k], preferred_element_type=jnp.float32).astype(jnp.bfloat16)
        q_buf[k, rows, :] = result[:, :head]
        kv[0, k, rows, :] = result[:, head:]

    def share_kv(k, part, first, count):
        rows = pl.ds(first, count)
        for d in range(1, pairs):
            there = (k + d) % pairs
            start(kv.at[0, k, rows, :], kv.at[d, there, rows, :], kv_s.at[d, k, part], kv_r.at[d, there, part], at_pair(d, 0))

    normalize(0)
    pass_q(0)
    for k in range(1, pairs):
        arrive(wq_rows(k, g), wz_s.at[k], wz_r.at[k])
        spread_q(k)
    finish_q(0)
    project(0, 0, tok)
    share_kv(0, 0, 0, tok)
    arrive(lat.at[1], lat_s.at[0], lat_r.at[0])
    normalize(1)
    project(0, tok, tok)
    share_kv(0, 1, tok, tok)
    pass_o(0, 0)
    for k, f in far:
        arrive(wo_rows((parity + f) % 2, k, g), oz_s.at[k * 2 + f], oz_r.at[k * 2 + f])
        spread_o(k, f)
    for k in range(1, pairs):
        pass_q(k)
        finish_q(k)
        project(k, 0, 2 * tok)
        share_kv(k, 0, 0, tok)
        share_kv(k, 1, tok, tok)

    def attend(k):
        for d in range(1, pairs):
            for part in range(2):
                arrive(kv.at[d, k, pl.ds(part * tok, tok), :], kv_s.at[d, k, part], kv_r.at[d, k, part])
        total = pairs * 2 * tok
        keys = kv[:, k, :, :head].reshape(total, head)
        values = kv[:, k, :, head:].reshape(total, head)
        cols = pl.ds(pl.multiple_of((parity * pairs + k) * head, head), head)
        for which in (1, 0):
            query = q_buf[k, pl.ds(which * tok, tok), :]
            scores = lax.dot_general(query, keys, (((1,), (1,)), ((), ())), preferred_element_type=jnp.float32)
            scores = scores / math.sqrt(head)
            largest = jnp.max(scores, axis=1, keepdims=True)
            weights = jnp.exp(scores - largest)
            probs = (weights / jnp.sum(weights, axis=1, keepdims=True)).astype(jnp.bfloat16)
            result = jnp.dot(probs, values, preferred_element_type=jnp.float32).astype(jnp.bfloat16)
            if which == 1:
                att_send[k] = result
                start(att_send.at[k], att_mine.at[:, cols], at_s.at[k], at_r.at[k], mate)
            else:
                att_mine[:, cols] = result

    for k in range(pairs):
        attend(k)
    for k, f in far:
        pass_o(k, f)
    finish_o(0, 0)
    for k, f in far:
        finish_o(k, f)
    for k in range(pairs):
        cols = pl.ds(pl.multiple_of(((1 - parity) * pairs + k) * head, head), head)
        arrive(att_mine.at[:, cols], at_s.at[k], at_r.at[k])

    @pl.loop(0, width // step)
    def _(i):
        cols = pl.ds(pl.multiple_of(i * step, step), step)
        total = jnp.dot(att_mine[...], wo[:, cols], preferred_element_type=jnp.float32)
        gate = mod[0:1, pl.ds(pl.multiple_of(2 * width + i * step, step), step)]
        out_ref[0, :, cols] = (gate * total).astype(jnp.bfloat16)

    for copy in sends:
        copy.wait_send()


def on_device(n_grp, n_sp, latents, timestep, w_mod, w_qkv, w_out):
    _, tok, width = latents.shape
    freq = w_mod.shape[0]
    head = w_qkv.shape[2] // 3
    pairs, chips = n_sp // 2, n_grp // 2
    embed = jnp.broadcast_to(embedding(timestep, freq), (16, freq))
    dma = pltpu.SemaphoreType.DMA
    bf16 = jnp.bfloat16
    anywhere = pl.BlockSpec(memory_space=pl.ANY)
    vmem = pl.BlockSpec(memory_space=pltpu.VMEM)
    return pl.pallas_call(
        functools.partial(kernel, n_grp, n_sp),
        out_shape=jax.ShapeDtypeStruct(latents.shape, bf16),
        in_specs=[anywhere, vmem, anywhere, anywhere, anywhere],
        out_specs=vmem,
        scratch_shapes=[
            pltpu.VMEM((2, tok, width), bf16),
            pltpu.VMEM(w_mod.shape, bf16),
            pltpu.VMEM((8, w_mod.shape[1]), jnp.float32),
            pltpu.VMEM((2 * tok, width), bf16),
            pltpu.VMEM((pairs, width, 3 * head), bf16),
            pltpu.VMEM((n_sp * head, width), bf16),
            pltpu.VMEM((pairs, 2 * tok, head), bf16),
            pltpu.VMEM((pairs, pairs, 2 * tok, 2 * head), bf16),
            pltpu.VMEM((tok, n_sp * head), bf16),
            pltpu.VMEM((pairs, tok, head), bf16),
            dma((4,)),
            dma((pairs,)),
            dma((pairs,)),
            dma((pairs, chips)),
            dma((pairs, chips)),
            dma((pairs, chips)),
            dma((pairs, chips)),
            dma((n_sp,)),
            dma((n_sp,)),
            dma((n_sp, chips)),
            dma((n_sp, chips)),
            dma((n_sp, chips)),
            dma((n_sp, chips)),
            dma((1,)),
            dma((1,)),
            dma((pairs, pairs, 2)),
            dma((pairs, pairs, 2)),
            dma((pairs,)),
            dma((pairs,)),
        ],
        compiler_params=pltpu.CompilerParams(
            collective_id=0, has_side_effects=True, vmem_limit_bytes=64000000
        ),
    )(latents, embed, w_mod, w_qkv, w_out)


def solution(mesh):
    placed = (P("grp", "sp", None), P("grp"), P(), P("sp", "grp", None), P("sp", "grp", None))
    body = functools.partial(on_device, mesh.shape["grp"], mesh.shape["sp"])
    return jax.shard_map(
        body, mesh=mesh, in_specs=placed, out_specs=P("grp", "sp", None), check_vma=False
    )
```

```python
import functools
import math

import jax
import jax.numpy as jnp
from jax import lax
from jax.experimental import pallas as pl
from jax.experimental.pallas import tpu as pltpu
from jax.sharding import PartitionSpec as P

MESH = pl.DeviceIdType.MESH
CHUNKS = 4


def embedding(timestep, freq):
    half_freq = freq // 2
    freqs = jnp.exp(-math.log(10000.0) * jnp.arange(half_freq, dtype=jnp.float32) / half_freq)
    angles = timestep.astype(jnp.float32)[:, None] * freqs[None, :]
    return jnp.concatenate([jnp.cos(angles), jnp.sin(angles)], axis=1).astype(jnp.bfloat16)


def kernel(
    n_grp,
    n_sp,
    lat_hbm,
    embed_ref,
    wmod_hbm,
    wqkv_hbm,
    wout_hbm,
    out_ref,
    lat,
    wmod,
    mod,
    normed,
    wq,
    wo,
    q_buf,
    kv,
    att_mine,
    att_send,
    loc_sem,
    wz_s,
    wz_r,
    wx_s,
    wx_r,
    wd_s,
    wd_r,
    oz_s,
    oz_r,
    ox_s,
    ox_r,
    od_s,
    od_r,
    lat_s,
    lat_r,
    kv_s,
    kv_r,
    at_s,
    at_r,
):
    g = lax.axis_index("grp")
    s = lax.axis_index("sp")
    core, chip = g % 2, g // 2
    chips = n_grp // 2
    pairs = n_sp // 2
    parity, pair = s % 2, s // 2
    tok, width = lat_hbm.shape[1], lat_hbm.shape[2]
    rows_q = wqkv_hbm.shape[1]
    rows_o = wout_hbm.shape[1]
    head = wqkv_hbm.shape[2] // 3
    sib = (chip * 2 + 1 - core, s)
    mate = (g, pair * 2 + 1 - parity)

    def at_chip(c):
        return ((chip + c) % chips * 2 + core, s)

    def at_pair(k, flip):
        return (g, (pair + k) % pairs * 2 + (parity + flip) % 2)

    def remote(src, dst, ssem, rsem, device):
        return pltpu.make_async_remote_copy(
            src_ref=src, dst_ref=dst, send_sem=ssem, recv_sem=rsem, device_id=device, device_id_type=MESH
        )

    def wq_rows(k, owner):
        return wq.at[k, pl.ds(pl.multiple_of(owner * rows_q, rows_q), rows_q), :]

    def wo_rows(par, k, owner):
        first = (par * pairs + k) * head + owner * rows_o
        return wo.at[pl.ds(pl.multiple_of(first, rows_o), rows_o), :]

    barrier = pltpu.get_barrier_semaphore()
    peers = [sib] + [at_chip(c) for c in range(1, chips)]
    peers += [at_pair(k, f) for k in range(pairs) for f in range(2) if (k, f) != (0, 0)]
    for peer in peers:
        pl.semaphore_signal(barrier, inc=1, device_id=peer, device_id_type=MESH)
    local = [
        pltpu.make_async_copy(wqkv_hbm.at[0], wq_rows(0, g), loc_sem.at[0]),
        pltpu.make_async_copy(wout_hbm.at[0], wo_rows(parity, 0, g), loc_sem.at[1]),
        pltpu.make_async_copy(lat_hbm.at[0], lat.at[0], loc_sem.at[2]),
        pltpu.make_async_copy(wmod_hbm, wmod, loc_sem.at[3]),
    ]
    for copy in local:
        copy.start()
    local[0].wait()
    local[1].wait()
    local[2].wait()
    pl.semaphore_wait(barrier, len(peers))

    sends = []

    def start(*args):
        copy = remote(*args)
        copy.start()
        sends.append(copy)

    def arrive(region, ssem, rsem):
        remote(region, region, ssem, rsem, sib).wait_recv()

    square = chips == 4
    near_x = chip // 2 * 2 + 1 - chip % 2
    near_y = (chip + 2) % 4
    corner = (near_x + 2) % 4
    to_x, to_y = (near_x * 2 + core, s), (near_y * 2 + core, s)
    others = [near_x, near_y, corner] if square else [(chip + chips - c) % chips for c in range(1, chips)]

    def q_part(k, owner, half):
        size = rows_q // 2
        return wq.at[k, pl.ds(pl.multiple_of(owner * rows_q + half * size, size), size), :]

    def o_part(par, k, owner, half):
        first = (par * pairs + k) * head + owner * rows_o
        size = width // 2
        return wo.at[pl.ds(pl.multiple_of(first, rows_o), rows_o), half * size : (half + 1) * size]

    class Spread:
        def __init__(self, i, whole, part, xs, xr, ds, dr):
            self.i, self.whole, self.part = i, whole, part
            self.xs, self.xr, self.ds, self.dr = xs, xr, ds, dr

        def cross(self, region, slot, device):
            start(region, region, self.xs.at[self.i, slot], self.xr.at[self.i, slot], device)

        def land(self, region, slot):
            arrive(region, self.xs.at[self.i, slot], self.xr.at[self.i, slot])

        def to_sib(self, region, slot):
            start(region, region, self.ds.at[self.i, slot], self.dr.at[self.i, slot], sib)

        def begin(self):
            mine = self.whole(g)
            if square:
                self.cross(mine, 0, to_x)
                self.cross(mine, 1, to_y)
            else:
                for c in range(1, chips):
                    self.cross(mine, c - 1, at_chip(c))
            self.to_sib(mine, 0)

        def relay(self):
            if square:
                for slot, device in ((0, to_y), (1, to_x)):
                    owner = others[slot] * 2 + core
                    self.land(self.whole(owner), slot)
                    self.cross(self.part(owner, slot), 2 + slot, device)
                    self.to_sib(self.whole(owner), 1 + slot)
            else:
                for slot in range(chips - 1):
                    region = self.whole(others[slot] * 2 + core)
                    self.land(region, slot)
                    self.to_sib(region, 1 + slot)

        def last(self):
            if square:
                owner = corner * 2 + core
                self.land(self.part(owner, 0), 2)
                self.land(self.part(owner, 1), 3)
                self.to_sib(self.whole(owner), 3)

        def finish(self):
            for slot, owner in enumerate([chip] + others):
                arrive(self.whole(owner * 2 + 1 - core), self.ds.at[self.i, slot], self.dr.at[self.i, slot])

    def spread_q(k):
        return Spread(k, functools.partial(wq_rows, k), functools.partial(q_part, k), wx_s, wx_r, wd_s, wd_r)

    def spread_o(k, flip):
        par = (parity + flip) % 2
        whole, part = functools.partial(wo_rows, par, k), functools.partial(o_part, par, k)
        return Spread(k * 2 + flip, whole, part, ox_s, ox_r, od_s, od_r)

    far = [(k, f) for k in range(pairs) for f in range(2) if (k, f) != (0, 0)]
    all_q = [spread_q(k) for k in range(pairs)]
    near_o, far_o = spread_o(0, 0), [spread_o(k, f) for k, f in far]

    def land_o(n):
        k, f = far[n]
        i = k * 2 + f
        arrive(wo_rows((parity + f) % 2, k, g), oz_s.at[i], oz_r.at[i])
        far_o[n].begin()

    all_q[0].begin()
    for k in range(1, pairs):
        start(wq_rows(0, g), wq_rows(k, g), wz_s.at[k], wz_r.at[k], at_pair(k, 0))
    for k, f in far:
        i = k * 2 + f
        start(wo_rows(parity, 0, g), wo_rows(parity, k, g), oz_s.at[i], oz_r.at[i], at_pair(k, f))
    piece = tok // CHUNKS
    for c in range(CHUNKS):
        rows = pl.ds(c * piece, piece)
        start(lat.at[0, rows, :], lat.at[1, rows, :], lat_s.at[c], lat_r.at[c], mate)
    near_o.begin()

    local[3].wait()
    step = min(512, width)

    @pl.loop(0, 3 * width // step)
    def _(i):
        cols = pl.ds(pl.multiple_of(i * step, step), step)
        part = jnp.dot(embed_ref[...], wmod[:, cols], preferred_element_type=jnp.float32)
        mod[:, cols] = part[:8]

    def normalize(which, first, count):
        block = 16

        @pl.loop(0, count // block)
        def _(i):
            rows = pl.ds(pl.multiple_of(first + i * block, block), block)
            values = lat[which, rows, :].astype(jnp.float32)
            center = jnp.mean(values, axis=-1, keepdims=True)
            values = values - center
            spread = jnp.mean(values * values, axis=-1, keepdims=True)
            scaled = values * lax.rsqrt(spread + 1e-06)
            shift = mod[0:1, 0:width]
            scale = mod[0:1, width : 2 * width]
            target = pl.ds(pl.multiple_of(which * tok + first + i * block, block), block)
            normed[target, :] = (scaled * (1.0 + scale) + shift).astype(jnp.bfloat16)

    def normalize_chunk(c):
        region = lat.at[1, pl.ds(c * piece, piece), :]
        arrive(region, lat_s.at[c], lat_r.at[c])
        normalize(1, c * piece, piece)

    spans = [(0, tok), (tok, tok - piece), (2 * tok - piece, piece)]

    def project(k, part):
        rows = pl.ds(*spans[part])
        result = jnp.dot(normed[rows, :], wq[k], preferred_element_type=jnp.float32).astype(jnp.bfloat16)
        q_buf[k, rows, :] = result[:, :head]
        kv[0, k, rows, :] = result[:, head:]

    def share_kv(k, part):
        rows = pl.ds(*spans[part])
        for d in range(1, pairs):
            there = (k + d) % pairs
            start(kv.at[0, k, rows, :], kv.at[d, there, rows, :], kv_s.at[d, k, part], kv_r.at[d, there, part], at_pair(d, 0))

    normalize(0, 0, tok)
    all_q[0].relay()
    near_o.relay()
    for k in range(1, pairs):
        arrive(wq_rows(k, g), wz_s.at[k], wz_r.at[k])
        all_q[k].begin()
    land_o(0)
    all_q[0].last()
    near_o.last()
    all_q[0].finish()
    project(0, 0)
    share_kv(0, 0)
    for k in range(1, pairs):
        all_q[k].relay()
    for n in range(1, len(far)):
        land_o(n)
    normalize_chunk(0)
    far_o[0].relay()
    for k in range(1, pairs):
        all_q[k].last()
        all_q[k].finish()
        project(k, 0)
        share_kv(k, 0)
    for c in range(1, CHUNKS - 1):
        normalize_chunk(c)
    for k in range(pairs):
        project(k, 1)
        share_kv(k, 1)
    for n in range(1, len(far)):
        far_o[n].relay()
    normalize_chunk(CHUNKS - 1)
    for k in range(pairs):
        project(k, 2)
        share_kv(k, 2)
    for spread in far_o:
        spread.last()

    def attend(k):
        for d in range(1, pairs):
            for part, span in enumerate(spans):
                arrive(kv.at[d, k, pl.ds(*span), :], kv_s.at[d, k, part], kv_r.at[d, k, part])
        total = pairs * 2 * tok
        keys = kv[:, k, :, :head].reshape(total, head)
        values = kv[:, k, :, head:].reshape(total, head)
        cols = pl.ds(pl.multiple_of((parity * pairs + k) * head, head), head)
        for which in (1, 0):
            query = q_buf[k, pl.ds(which * tok, tok), :]
            scores = lax.dot_general(query, keys, (((1,), (1,)), ((), ())), preferred_element_type=jnp.float32)
            scores = scores / math.sqrt(head)
            largest = jnp.max(scores, axis=1, keepdims=True)
            weights = jnp.exp(scores - largest)
            probs = (weights / jnp.sum(weights, axis=1, keepdims=True)).astype(jnp.bfloat16)
            result = jnp.dot(probs, values, preferred_element_type=jnp.float32).astype(jnp.bfloat16)
            if which == 1:
                att_send[k] = result
                start(att_send.at[k], att_mine.at[:, cols], at_s.at[k], at_r.at[k], mate)
            else:
                att_mine[:, cols] = result

    for k in range(pairs):
        attend(k)
    for spread in [near_o] + far_o:
        spread.finish()
    for k in range(pairs):
        cols = pl.ds(pl.multiple_of(((1 - parity) * pairs + k) * head, head), head)
        arrive(att_mine.at[:, cols], at_s.at[k], at_r.at[k])

    @pl.loop(0, width // step)
    def _(i):
        cols = pl.ds(pl.multiple_of(i * step, step), step)
        total = jnp.dot(att_mine[...], wo[:, cols], preferred_element_type=jnp.float32)
        gate = mod[0:1, pl.ds(pl.multiple_of(2 * width + i * step, step), step)]
        out_ref[0, :, cols] = (gate * total).astype(jnp.bfloat16)

    for copy in sends:
        copy.wait_send()


def on_device(n_grp, n_sp, latents, timestep, w_mod, w_qkv, w_out):
    _, tok, width = latents.shape
    freq = w_mod.shape[0]
    head = w_qkv.shape[2] // 3
    pairs, chips = n_sp // 2, n_grp // 2
    embed = jnp.broadcast_to(embedding(timestep, freq), (16, freq))
    dma = pltpu.SemaphoreType.DMA
    bf16 = jnp.bfloat16
    anywhere = pl.BlockSpec(memory_space=pl.ANY)
    vmem = pl.BlockSpec(memory_space=pltpu.VMEM)
    return pl.pallas_call(
        functools.partial(kernel, n_grp, n_sp),
        out_shape=jax.ShapeDtypeStruct(latents.shape, bf16),
        in_specs=[anywhere, vmem, anywhere, anywhere, anywhere],
        out_specs=vmem,
        scratch_shapes=[
            pltpu.VMEM((2, tok, width), bf16),
            pltpu.VMEM(w_mod.shape, bf16),
            pltpu.VMEM((8, w_mod.shape[1]), jnp.float32),
            pltpu.VMEM((2 * tok, width), bf16),
            pltpu.VMEM((pairs, width, 3 * head), bf16),
            pltpu.VMEM((n_sp * head, width), bf16),
            pltpu.VMEM((pairs, 2 * tok, head), bf16),
            pltpu.VMEM((pairs, pairs, 2 * tok, 2 * head), bf16),
            pltpu.VMEM((tok, n_sp * head), bf16),
            pltpu.VMEM((pairs, tok, head), bf16),
            dma((4,)),
            dma((pairs,)),
            dma((pairs,)),
            dma((pairs, chips)),
            dma((pairs, chips)),
            dma((pairs, chips)),
            dma((pairs, chips)),
            dma((n_sp,)),
            dma((n_sp,)),
            dma((n_sp, chips)),
            dma((n_sp, chips)),
            dma((n_sp, chips)),
            dma((n_sp, chips)),
            dma((CHUNKS,)),
            dma((CHUNKS,)),
            dma((pairs, pairs, 3)),
            dma((pairs, pairs, 3)),
            dma((pairs,)),
            dma((pairs,)),
        ],
        compiler_params=pltpu.CompilerParams(
            collective_id=0, has_side_effects=True, vmem_limit_bytes=64000000
        ),
    )(latents, embed, w_mod, w_qkv, w_out)


def solution(mesh):
    placed = (P("grp", "sp", None), P("grp"), P(), P("sp", "grp", None), P("sp", "grp", None))
    body = functools.partial(on_device, mesh.shape["grp"], mesh.shape["sp"])
    return jax.shard_map(
        body, mesh=mesh, in_specs=placed, out_specs=P("grp", "sp", None), check_vma=False
    )
```

```python
import functools
import math

import jax
import jax.numpy as jnp
from jax import lax
from jax.experimental import pallas as pl
from jax.experimental.pallas import tpu as pltpu
from jax.sharding import PartitionSpec as P

MESH = pl.DeviceIdType.MESH
CHUNKS = 4


def embedding(timestep, freq):
    half_freq = freq // 2
    freqs = jnp.exp(-math.log(10000.0) * jnp.arange(half_freq, dtype=jnp.float32) / half_freq)
    angles = timestep.astype(jnp.float32)[:, None] * freqs[None, :]
    return jnp.cos(angles), jnp.sin(angles)


def kernel(
    n_grp,
    n_sp,
    lat_hbm,
    cos_ref,
    sin_ref,
    wmod_hbm,
    wqkv_hbm,
    wout_hbm,
    out_hbm,
    lat,
    wmod,
    mod,
    normed,
    wq,
    wo,
    q_buf,
    kv,
    att_mine,
    att_send,
    out_buf,
    loc_sem,
    wz_s,
    wz_r,
    wx_s,
    wx_r,
    wd_s,
    wd_r,
    oz_s,
    oz_r,
    ox_s,
    ox_r,
    od_s,
    od_r,
    lat_s,
    lat_r,
    kv_s,
    kv_r,
    at_s,
    at_r,
):
    g = lax.axis_index("grp")
    s = lax.axis_index("sp")
    core, chip = g % 2, g // 2
    chips = n_grp // 2
    pairs = n_sp // 2
    parity, pair = s % 2, s // 2
    tok, width = lat_hbm.shape[1], lat_hbm.shape[2]
    rows_q = wqkv_hbm.shape[1]
    rows_o = wout_hbm.shape[1]
    head = wqkv_hbm.shape[2] // 3
    sib = (chip * 2 + 1 - core, s)
    mate = (g, pair * 2 + 1 - parity)

    def at_chip(c):
        return ((chip + c) % chips * 2 + core, s)

    def at_pair(k, flip):
        return (g, (pair + k) % pairs * 2 + (parity + flip) % 2)

    def remote(src, dst, ssem, rsem, device):
        return pltpu.make_async_remote_copy(
            src_ref=src, dst_ref=dst, send_sem=ssem, recv_sem=rsem, device_id=device, device_id_type=MESH
        )

    def wq_rows(k, owner):
        return wq.at[k, pl.ds(pl.multiple_of(owner * rows_q, rows_q), rows_q), :]

    def wo_rows(par, k, owner):
        first = (par * pairs + k) * head + owner * rows_o
        return wo.at[pl.ds(pl.multiple_of(first, rows_o), rows_o), :]

    barrier = pltpu.get_barrier_semaphore()
    peers = [sib] + [at_chip(c) for c in range(1, chips)]
    peers += [at_pair(k, f) for k in range(pairs) for f in range(2) if (k, f) != (0, 0)]
    for peer in peers:
        pl.semaphore_signal(barrier, inc=1, device_id=peer, device_id_type=MESH)
    local = [
        pltpu.make_async_copy(wqkv_hbm.at[0], wq_rows(0, g), loc_sem.at[0]),
        pltpu.make_async_copy(wout_hbm.at[0], wo_rows(parity, 0, g), loc_sem.at[1]),
        pltpu.make_async_copy(lat_hbm.at[0], lat.at[0], loc_sem.at[2]),
        pltpu.make_async_copy(wmod_hbm, wmod, loc_sem.at[3]),
    ]
    for copy in local:
        copy.start()
    local[0].wait()
    local[1].wait()
    local[2].wait()
    pl.semaphore_wait(barrier, len(peers))

    sends = []

    def start(*args):
        copy = remote(*args)
        copy.start()
        sends.append(copy)

    def arrive(region, ssem, rsem):
        remote(region, region, ssem, rsem, sib).wait_recv()

    square = chips == 4
    near_x = chip // 2 * 2 + 1 - chip % 2
    near_y = (chip + 2) % 4
    corner = (near_x + 2) % 4
    to_x, to_y = (near_x * 2 + core, s), (near_y * 2 + core, s)
    others = [near_x, near_y, corner] if square else [(chip + chips - c) % chips for c in range(1, chips)]

    def q_part(k, owner, half):
        size = rows_q // 2
        return wq.at[k, pl.ds(pl.multiple_of(owner * rows_q + half * size, size), size), :]

    def o_part(par, k, owner, half):
        first = (par * pairs + k) * head + owner * rows_o
        size = width // 2
        return wo.at[pl.ds(pl.multiple_of(first, rows_o), rows_o), half * size : (half + 1) * size]

    class Spread:
        def __init__(self, i, whole, part, xs, xr, ds, dr):
            self.i, self.whole, self.part = i, whole, part
            self.xs, self.xr, self.ds, self.dr = xs, xr, ds, dr

        def cross(self, region, slot, device):
            start(region, region, self.xs.at[self.i, slot], self.xr.at[self.i, slot], device)

        def land(self, region, slot):
            arrive(region, self.xs.at[self.i, slot], self.xr.at[self.i, slot])

        def to_sib(self, region, slot):
            start(region, region, self.ds.at[self.i, slot], self.dr.at[self.i, slot], sib)

        def begin(self):
            mine = self.whole(g)
            if square:
                self.cross(mine, 0, to_x)
                self.cross(mine, 1, to_y)
            else:
                for c in range(1, chips):
                    self.cross(mine, c - 1, at_chip(c))
            self.to_sib(mine, 0)

        def relay(self):
            if square:
                for slot, device in ((0, to_y), (1, to_x)):
                    owner = others[slot] * 2 + core
                    self.land(self.whole(owner), slot)
                    self.cross(self.part(owner, slot), 2 + slot, device)
                    self.to_sib(self.whole(owner), 1 + slot)
            else:
                for slot in range(chips - 1):
                    region = self.whole(others[slot] * 2 + core)
                    self.land(region, slot)
                    self.to_sib(region, 1 + slot)

        def last(self):
            if square:
                owner = corner * 2 + core
                self.land(self.part(owner, 0), 2)
                self.land(self.part(owner, 1), 3)
                self.to_sib(self.whole(owner), 3)

        def finish(self):
            for slot, owner in enumerate([chip] + others):
                arrive(self.whole(owner * 2 + 1 - core), self.ds.at[self.i, slot], self.dr.at[self.i, slot])

    def spread_q(k):
        return Spread(k, functools.partial(wq_rows, k), functools.partial(q_part, k), wx_s, wx_r, wd_s, wd_r)

    def spread_o(k, flip):
        par = (parity + flip) % 2
        whole, part = functools.partial(wo_rows, par, k), functools.partial(o_part, par, k)
        return Spread(k * 2 + flip, whole, part, ox_s, ox_r, od_s, od_r)

    far = [(k, f) for k in range(pairs) for f in range(2) if (k, f) != (0, 0)]
    all_q = [spread_q(k) for k in range(pairs)]
    near_o, far_o = spread_o(0, 0), [spread_o(k, f) for k, f in far]

    def land_o(n):
        k, f = far[n]
        i = k * 2 + f
        arrive(wo_rows((parity + f) % 2, k, g), oz_s.at[i], oz_r.at[i])
        far_o[n].begin()

    all_q[0].begin()
    for k in range(1, pairs):
        start(wq_rows(0, g), wq_rows(k, g), wz_s.at[k], wz_r.at[k], at_pair(k, 0))

    def send_o(n):
        for k, f in far[n : n + 1]:
            i = k * 2 + f
            start(wo_rows(parity, 0, g), wo_rows(parity, k, g), oz_s.at[i], oz_r.at[i], at_pair(k, f))

    piece = tok // CHUNKS

    def send_chunk(c):
        rows = pl.ds(c * piece, piece)
        start(lat.at[0, rows, :], lat.at[1, rows, :], lat_s.at[c], lat_r.at[c], mate)

    send_chunk(0)

    local[3].wait()
    step = min(512, width)
    embed = jnp.concatenate([cos_ref[...], sin_ref[...]], axis=1).astype(jnp.bfloat16)
    embed = jnp.broadcast_to(embed, (16, embed.shape[1]))

    @pl.loop(0, 3 * width // step)
    def _(i):
        cols = pl.ds(pl.multiple_of(i * step, step), step)
        part = jnp.dot(embed, wmod[:, cols], preferred_element_type=jnp.float32)
        mod[:, cols] = part[:8]

    def normalize(which, first, count):
        block = 16

        @pl.loop(0, count // block)
        def _(i):
            rows = pl.ds(pl.multiple_of(first + i * block, block), block)
            values = lat[which, rows, :].astype(jnp.float32)
            center = jnp.mean(values, axis=-1, keepdims=True)
            values = values - center
            spread = jnp.mean(values * values, axis=-1, keepdims=True)
            scaled = values * lax.rsqrt(spread + 1e-06)
            shift = mod[0:1, 0:width]
            scale = mod[0:1, width : 2 * width]
            target = pl.ds(pl.multiple_of(which * tok + first + i * block, block), block)
            normed[target, :] = (scaled * (1.0 + scale) + shift).astype(jnp.bfloat16)

    def normalize_chunk(c):
        region = lat.at[1, pl.ds(c * piece, piece), :]
        arrive(region, lat_s.at[c], lat_r.at[c])
        normalize(1, c * piece, piece)

    spans = [(0, tok), (tok, tok - piece), (2 * tok - piece, piece)]

    def project(k, part):
        rows = pl.ds(*spans[part])
        result = jnp.dot(normed[rows, :], wq[k], preferred_element_type=jnp.float32).astype(jnp.bfloat16)
        q_buf[k, rows, :] = result[:, :head]
        kv[0, k, rows, :] = result[:, head:]

    def share_kv(k, part):
        rows = pl.ds(*spans[part])
        for d in range(1, pairs):
            there = (k + d) % pairs
            start(kv.at[0, k, rows, :], kv.at[d, there, rows, :], kv_s.at[d, k, part], kv_r.at[d, there, part], at_pair(d, 0))

    normalize(0, 0, tok)
    all_q[0].relay()
    near_o.begin()
    send_chunk(1)
    for k in range(1, pairs):
        arrive(wq_rows(k, g), wz_s.at[k], wz_r.at[k])
        all_q[k].begin()
    send_o(0)
    send_chunk(2)
    send_o(1)
    send_chunk(3)
    for n in range(2, len(far)):
        send_o(n)
    all_q[0].last()
    near_o.relay()
    all_q[0].finish()
    project(0, 0)
    share_kv(0, 0)
    near_o.last()
    for k in range(1, pairs):
        all_q[k].relay()
    normalize_chunk(0)
    for k in range(1, pairs):
        all_q[k].last()
        all_q[k].finish()
        project(k, 0)
        share_kv(k, 0)
    land_o(0)
    land_o(1)
    for c in range(1, CHUNKS - 1):
        normalize_chunk(c)
    for k in range(pairs):
        project(k, 1)
        share_kv(k, 1)
    normalize_chunk(CHUNKS - 1)
    for k in range(pairs):
        project(k, 2)
        share_kv(k, 2)
    far_o[0].relay()
    for n in range(2, len(far)):
        land_o(n)
    far_o[1].relay()
    far_o[0].last()

    def attend(k):
        for d in range(1, pairs):
            for part, span in enumerate(spans):
                arrive(kv.at[d, k, pl.ds(*span), :], kv_s.at[d, k, part], kv_r.at[d, k, part])
        total = pairs * 2 * tok
        keys = kv[:, k, :, :head].reshape(total, head)
        values = kv[:, k, :, head:].reshape(total, head)
        cols = pl.ds(pl.multiple_of((parity * pairs + k) * head, head), head)
        for which in (1, 0):
            query = q_buf[k, pl.ds(which * tok, tok), :]
            scores = lax.dot_general(query, keys, (((1,), (1,)), ((), ())), preferred_element_type=jnp.float32)
            scores = scores / math.sqrt(head)
            largest = jnp.max(scores, axis=1, keepdims=True)
            weights = jnp.exp(scores - largest)
            probs = (weights / jnp.sum(weights, axis=1, keepdims=True)).astype(jnp.bfloat16)
            result = jnp.dot(probs, values, preferred_element_type=jnp.float32).astype(jnp.bfloat16)
            if which == 1:
                att_send[k] = result
                start(att_send.at[k], att_mine.at[:, cols], at_s.at[k], at_r.at[k], mate)
            else:
                att_mine[:, cols] = result

    attend(0)
    for spread in far_o[2:]:
        spread.relay()
    far_o[1].last()
    for k in range(1, pairs):
        attend(k)
    for spread in far_o[2:]:
        spread.last()
    for spread in [near_o] + far_o:
        spread.finish()
    for k in range(pairs):
        cols = pl.ds(pl.multiple_of(((1 - parity) * pairs + k) * head, head), head)
        arrive(att_mine.at[:, cols], at_s.at[k], at_r.at[k])
    outs = []
    for i in range(width // step):
        cols = slice(i * step, (i + 1) * step)
        total = jnp.dot(att_mine[...], wo[:, cols], preferred_element_type=jnp.float32)
        gate = mod[0:1, 2 * width + i * step : 2 * width + (i + 1) * step]
        out_buf[:, cols] = (gate * total).astype(jnp.bfloat16)
        outs.append(pltpu.make_async_copy(out_buf.at[:, cols], out_hbm.at[0, :, cols], loc_sem.at[4 + i]))
        outs[i].start()
    for copy in outs:
        copy.wait()
    for copy in sends:
        copy.wait_send()


def on_device(n_grp, n_sp, latents, timestep, w_mod, w_qkv, w_out):
    _, tok, width = latents.shape
    freq = w_mod.shape[0]
    head = w_qkv.shape[2] // 3
    pairs, chips = n_sp // 2, n_grp // 2
    cos, sin = embedding(timestep, freq)
    dma = pltpu.SemaphoreType.DMA
    bf16 = jnp.bfloat16
    anywhere = pl.BlockSpec(memory_space=pl.ANY)
    vmem = pl.BlockSpec(memory_space=pltpu.VMEM)
    return pl.pallas_call(
        functools.partial(kernel, n_grp, n_sp),
        out_shape=jax.ShapeDtypeStruct(latents.shape, bf16),
        in_specs=[anywhere, vmem, vmem, anywhere, anywhere, anywhere],
        out_specs=anywhere,
        scratch_shapes=[
            pltpu.VMEM((2, tok, width), bf16),
            pltpu.VMEM(w_mod.shape, bf16),
            pltpu.VMEM((8, w_mod.shape[1]), jnp.float32),
            pltpu.VMEM((2 * tok, width), bf16),
            pltpu.VMEM((pairs, width, 3 * head), bf16),
            pltpu.VMEM((n_sp * head, width), bf16),
            pltpu.VMEM((pairs, 2 * tok, head), bf16),
            pltpu.VMEM((pairs, pairs, 2 * tok, 2 * head), bf16),
            pltpu.VMEM((tok, n_sp * head), bf16),
            pltpu.VMEM((pairs, tok, head), bf16),
            pltpu.VMEM((tok, width), bf16),
            dma((4 + width // min(512, width),)),
            dma((pairs,)),
            dma((pairs,)),
            dma((pairs, chips)),
            dma((pairs, chips)),
            dma((pairs, chips)),
            dma((pairs, chips)),
            dma((n_sp,)),
            dma((n_sp,)),
            dma((n_sp, chips)),
            dma((n_sp, chips)),
            dma((n_sp, chips)),
            dma((n_sp, chips)),
            dma((CHUNKS,)),
            dma((CHUNKS,)),
            dma((pairs, pairs, 3)),
            dma((pairs, pairs, 3)),
            dma((pairs,)),
            dma((pairs,)),
        ],
        compiler_params=pltpu.CompilerParams(
            collective_id=0, has_side_effects=True, vmem_limit_bytes=64000000
        ),
    )(latents, cos, sin, w_mod, w_qkv, w_out)


def solution(mesh):
    placed = (P("grp", "sp", None), P("grp"), P(), P("sp", "grp", None), P("sp", "grp", None))
    body = functools.partial(on_device, mesh.shape["grp"], mesh.shape["sp"])
    return jax.shard_map(
        body, mesh=mesh, in_specs=placed, out_specs=P("grp", "sp", None), check_vma=False
    )
```
